32 devices in a mesh: mod: 2 (over y), exp: 16 (over z, x, core).
Axes of the slice: x: 2, y: 2, z: 4, core: 2. Of those that a mesh axis runs over, the one named last changes fastest.
Arguments:
- tokens: bfloat16 [2, 8192, 1024], P('mod', 'exp'), may hold values from -60 to 60
- bottleneck: bfloat16 [64, 4, 1024], P('exp'), may hold values from -6 to 6
- clip_ids: int32 [2, 8192], P('mod', 'exp'), may hold values from 0 to 63, as said below
- expert_ids: int32 [2, 8192], P('mod', 'exp'), may hold values from 0 to 15, as said below
- slots: int32 [2, 8192], P('mod', 'exp'), may hold values from 0 to 127, as said below
- norm1_gain: bfloat16 [2, 1024], P('mod'), may hold values from 0.099609375 to 1.8984375
- attn_qkv: bfloat16 [2, 1024, 3072], P('mod'), may hold values from -2 to 2
- attn_out: bfloat16 [2, 1024, 1024], P('mod'), may hold values from -0.1875 to 0.1875
- norm2_gain: bfloat16 [2, 1024], P('mod'), may hold values from 0.099609375 to 1.8984375
- router: bfloat16 [1024, 16], replicated, may hold values from -0.1875 to 0.1875
- fc_in: bfloat16 [16, 1024, 4096], P('exp'), may hold values from -0.1875 to 0.1875
- fc_out: bfloat16 [16, 4096, 1024], P('exp'), may hold values from -0.09375 to 0.09375
Outputs:
- mixed_tokens: bfloat16 [2, 8192, 1024], P('mod', 'exp')
- new_bottleneck: bfloat16 [64, 4, 1024], P('exp')
The draws below stay inside these ranges and needn't reach their ends.
Inputs may be any that keep to these rules, and one draw needn't show every extreme that they name: `clip_ids`: Non-decreasing in each modality; the tokens of block b of 512 rows belong to clips b * 4 to (b + 1) * 4 - 1, each of which has one or more of them. `expert_ids`: each token's single expert. For the k tokens of one block of 512 rows of one modality that share an expert, the slots are 0 to k - 1 in some order; k is at most 128; in every block of each modality one expert, the same for all blocks of that modality, has k = 128.
All inputs are finite; a program needn't handle non-finite values.
Results may differ from the reference program's by a relative error of at most 0.0085.
Values may be sent and summed in bfloat16 or wider, within the bound.
A program may use at most 128 MiB of HBM per device.

```python
import math
import jax
import jax.numpy as jnp
from jax import lax

D = 1024
FF = 4096
HEAD = 64
NB = 4
TOK_DEV = 512
CLIPS_DEV = 4
EXPERTS = 16
TOKENS = 8192
CLIPS = 64
CAP = 64


def routing_table(key):
    blocks = TOKENS // TOK_DEV
    queue_len = 2 * CAP
    seat_count = EXPERTS * queue_len
    routing_key = jax.random.fold_in(key, 7001)
    hot_key, level_key, block_key = jax.random.split(routing_key, 3)
    hottest = jax.random.randint(hot_key, (2,), 0, EXPERTS)
    levels = jax.random.randint(level_key, (2, EXPERTS), 0, 4)
    block_seeds = jax.random.split(block_key, 2 * blocks)
    modality_of = jnp.arange(2 * blocks, dtype=jnp.int32) // blocks
    seat_index = jnp.arange(seat_count, dtype=jnp.int32)
    seat_expert = seat_index // queue_len

    def one_block(block_seed, modality):
        second_key, noise_key, order_key = jax.random.split(block_seed, 3)
        second = jax.random.randint(second_key, (), 0, EXPERTS)
        jitter = jax.random.randint(noise_key, (seat_count,), 0, 4096)
        favoured = (seat_expert == hottest[modality]) | (seat_expert == second)
        seat_score = jitter + levels[modality][seat_expert] * 1024 + jnp.where(favoured, 16384, 0)
        ranked = seat_score * seat_count + seat_index
        picked = lax.top_k(ranked, TOK_DEV)[1]
        marked = jnp.zeros((seat_count,), jnp.int32).at[picked].set(1)
        grouped = marked.reshape(EXPERTS, queue_len)
        rank_table = (jnp.cumsum(grouped, axis=1) - grouped).reshape(seat_count)
        token_order = jax.random.permutation(order_key, TOK_DEV)
        assigned = picked[token_order]
        return (seat_expert[assigned], rank_table[assigned])
    experts_drawn, slots_drawn = jax.vmap(one_block)(block_seeds, modality_of)
    return (experts_drawn.reshape(2, TOKENS).astype(jnp.int32), slots_drawn.reshape(2, TOKENS).astype(jnp.int32))


def draw_expert_ids(key, part):
    return routing_table(key)[0]


def draw_slots(key, part):
    return routing_table(key)[1]


def draw_clip_ids(key, part):
    blocks = TOKENS // TOK_DEV
    block_seeds = jax.random.split(jax.random.fold_in(key, 7002), 2 * blocks)
    position = jnp.arange(TOK_DEV, dtype=jnp.int32)

    def one_block(block_seed):
        cuts = jax.random.permutation(block_seed, TOK_DEV - 1)[:CLIPS_DEV - 1] + 1
        return jnp.sum((position[:, None] >= cuts[None, :]).astype(jnp.int32), axis=1)
    local_ids = jax.vmap(one_block)(block_seeds).reshape(2, blocks, TOK_DEV)
    offsets = jnp.arange(blocks, dtype=jnp.int32)[None, :, None] * CLIPS_DEV
    return (local_ids + offsets).reshape(2, TOKENS).astype(jnp.int32)


def draw_tokens(key, part):
    normal_draw = jnp.clip(jax.random.normal(key, (2, TOKENS, D), jnp.float32), -6.0, 6.0)
    return normal_draw.astype(jnp.bfloat16)


def draw_attn_qkv(key, part):
    unit_scale = 1.0 / math.sqrt(D)
    entries = jax.random.normal(key, (2, D, 3 * D), jnp.float32) * unit_scale
    return jnp.clip(entries, -2.0, 2.0).astype(jnp.bfloat16)


def shard_levels(stream_key, shape, pieces, smallest, top_value):
    gain = 1.0
    for dim, parts in pieces:
        steps = jax.random.uniform(jax.random.fold_in(jax.random.fold_in(stream_key, 6), dim), (parts,), jnp.float32, smallest / len(pieces), top_value / len(pieces))
        gain = gain * jnp.repeat(jnp.exp(steps), shape[dim] // parts).reshape((-1,) + (1,) * (len(shape) - 1 - dim))
    return gain


def scatter_about(stream_key, shape, scale, limit, cuts=(), kind=jnp.bfloat16):
    factor_of = shard_levels(stream_key, shape, cuts, -0.22, 0.18) if cuts else 1.0
    values = jax.random.normal(stream_key, shape, jnp.float32) * scale * factor_of
    return jnp.minimum(jnp.maximum(values, -limit), limit).astype(kind)


def setup_inputs(seed: int = 0) -> dict:
    key_list = jax.random.split(jax.random.key(seed), 13)
    return {
        "tokens": draw_tokens(jax.random.fold_in(key_list[12], 71), 0),
        "bottleneck": scatter_about(key_list[1], (CLIPS, NB, D), 1.0, 6.0, ((0, 16),)),
        "clip_ids": draw_clip_ids(jax.random.fold_in(key_list[12], 71), 0),
        "expert_ids": draw_expert_ids(jax.random.fold_in(key_list[12], 71), 0),
        "slots": draw_slots(jax.random.fold_in(key_list[12], 71), 0),
        "norm1_gain": jnp.clip(1.0 + 0.18 * jax.random.normal(key_list[5], (2, D), jnp.float32), 0.099609375, 1.8984375).astype(jnp.bfloat16),
        "attn_qkv": draw_attn_qkv(jax.random.fold_in(key_list[12], 71), 0),
        "attn_out": scatter_about(key_list[7], (2, D, D), D ** -0.5, 0.1875, ((0, 2),)),
        "norm2_gain": jnp.clip(1.0 + 0.18 * jax.random.normal(key_list[8], (2, D), jnp.float32), 0.099609375, 1.8984375).astype(jnp.bfloat16),
        "router": scatter_about(key_list[9], (D, EXPERTS), D ** -0.5, 0.1875),
        "fc_in": scatter_about(key_list[10], (EXPERTS, D, FF), D ** -0.5, 0.1875, ((0, 16),)),
        "fc_out": scatter_about(key_list[11], (EXPERTS, FF, D), FF ** -0.5, 0.09375, ((0, 16),)),
    }


EPSILON = 1e-06

def layer_norm(features, scales):
    row_mean = lax.optimization_barrier(jnp.mean(features, axis=-1, keepdims=True))
    centred = features - row_mean
    spread = lax.optimization_barrier(jnp.mean(centred * centred, axis=-1, keepdims=True))
    return centred * lax.rsqrt(spread + EPSILON) * scales.astype(jnp.float32)

def attend(token_rows, latent_rows, token_clip, clip_start, scales, w_qkv, w_out):
    n_clips, n_latent, model_width = latent_rows.shape
    n_tokens = token_rows.shape[0]
    all_rows = jnp.concatenate([token_rows, latent_rows.reshape(n_clips * n_latent, model_width)], axis=0)
    row_count = all_rows.shape[0]
    head_count = model_width // HEAD
    normed = layer_norm(all_rows.astype(jnp.float32), scales).astype(jnp.bfloat16)
    packed = jnp.dot(normed, w_qkv, preferred_element_type=jnp.float32).astype(jnp.bfloat16)
    queries = packed[:, :model_width].reshape(row_count, head_count, HEAD)
    key_rows = packed[:, model_width:2 * model_width].reshape(row_count, head_count, HEAD)
    value_rows = packed[:, 2 * model_width:].reshape(row_count, head_count, HEAD)
    latent_clip = clip_start + jnp.arange(n_clips * n_latent, dtype=jnp.int32) // n_latent
    row_clip = jnp.concatenate([token_clip.astype(jnp.int32), latent_clip.astype(jnp.int32)])
    allowed = row_clip[:, None] == row_clip[None, :]
    scores = jnp.einsum('qhd,khd->hqk', queries.astype(jnp.float32), key_rows.astype(jnp.float32)) * (1.0 / math.sqrt(HEAD))
    scores = jnp.where(allowed[None, :, :], scores, -jnp.inf)
    row_max = lax.optimization_barrier(jnp.max(scores, axis=-1, keepdims=True))
    weights = jnp.exp(scores - row_max)
    attn_weights = (weights / lax.optimization_barrier(jnp.sum(weights, axis=-1, keepdims=True))).astype(jnp.bfloat16)
    attended = jnp.einsum('hqk,khd->qhd', attn_weights.astype(jnp.float32), value_rows.astype(jnp.float32))
    attended = attended.reshape(row_count, model_width).astype(jnp.bfloat16)
    updated = all_rows.astype(jnp.float32) + jnp.dot(attended, w_out, preferred_element_type=jnp.float32)
    return (updated[:n_tokens], updated[n_tokens:].reshape(n_clips, n_latent, model_width))

def expert_step(operands):
    block_rows, weight_in, weight_out = operands
    hidden_units = jnp.dot(block_rows, weight_in, preferred_element_type=jnp.float32)
    activated = jax.nn.gelu(hidden_units, approximate=False).astype(jnp.bfloat16)
    return jnp.dot(activated, weight_out, preferred_element_type=jnp.float32).astype(jnp.bfloat16)

def reference(tokens, bottleneck, clip_ids, expert_ids, slots, norm1_gain, attn_qkv, attn_out, norm2_gain, router, fc_in, fc_out):
    model_width = tokens.shape[-1]
    blocks = tokens.shape[1] // TOK_DEV
    latent = bottleneck.reshape(blocks, CLIPS_DEV, NB, model_width)
    starts = jnp.arange(blocks, dtype=jnp.int32) * CLIPS_DEV
    block_of = jnp.arange(blocks * TOK_DEV, dtype=jnp.int32) // TOK_DEV
    column = jnp.arange(EXPERTS, dtype=jnp.int32)
    slot_total = EXPERTS * blocks * CAP
    outputs = []
    latents = []
    for modality in range(2):

        def one_block(operands):
            token_rows, latent_rows, token_clip, clip_start = operands
            return attend(token_rows, latent_rows, token_clip, clip_start, norm1_gain[modality], attn_qkv[modality], attn_out[modality])
        mid_tokens, mid_latent = lax.map(one_block, (tokens[modality].reshape(blocks, TOK_DEV, model_width), latent, clip_ids[modality].reshape(blocks, TOK_DEV), starts))
        mid_tokens = mid_tokens.reshape(blocks * TOK_DEV, model_width)
        latents.append(mid_latent)
        expert_in = layer_norm(mid_tokens, norm2_gain[modality]).astype(jnp.bfloat16)
        logits = jnp.dot(expert_in, router, preferred_element_type=jnp.float32)
        chosen = expert_ids[modality].astype(jnp.int32)
        slot_ids = slots[modality].astype(jnp.int32)
        picked = lax.optimization_barrier(jnp.sum(jnp.where(column[None, :] == chosen[:, None], logits, jnp.zeros_like(logits)), axis=1))
        gate_value = jax.nn.sigmoid(picked)
        served = slot_ids < CAP
        position = jnp.where(served, chosen * (blocks * CAP) + block_of * CAP + slot_ids, slot_total).astype(jnp.int32)
        buffer = jnp.zeros((slot_total, model_width), jnp.bfloat16).at[position].set(expert_in, mode='drop')
        served_rows = lax.map(expert_step, (buffer.reshape(EXPERTS, blocks * CAP, model_width), fc_in, fc_out))
        served_rows = served_rows.reshape(slot_total, model_width)
        returned = jnp.take(served_rows, position, axis=0, mode='fill', fill_value=0)
        outputs.append((mid_tokens + gate_value[:, None] * returned.astype(jnp.float32)).astype(jnp.bfloat16))
    mixed_tokens = jnp.stack(outputs)
    new_bottleneck = ((latents[0] + latents[1]) * 0.5).astype(jnp.bfloat16).reshape(blocks * CLIPS_DEV, NB, model_width)
    return (mixed_tokens, new_bottleneck)
```

```python
import functools
import math

import jax
import jax.numpy as jnp
from jax import lax
from jax.experimental import pallas as pl
from jax.experimental.pallas import tpu as pltpu
from jax.sharding import PartitionSpec as P

MESH = pl.DeviceIdType.MESH
HEAD = 64
CAP_FACTOR = 2
EARLY = 128
PAIRS = 2
NEAR = 4


EPSILON = 1e-06


def layer_norm(features, scales):
    row_mean = jnp.mean(features, axis=-1, keepdims=True)
    centred = features - row_mean
    spread = jnp.mean(centred * centred, axis=-1, keepdims=True)
    return centred * lax.rsqrt(spread + EPSILON) * scales


def gelu(x):
    half = 0.5 * x
    return half + half * lax.erf(x * (1.0 / math.sqrt(2.0)))


def matmul(lhs, rhs):
    return jnp.dot(lhs, rhs, preferred_element_type=jnp.float32)


def one_hot(condition):
    return jnp.where(condition, 1.0, 0.0).astype(jnp.bfloat16)


def to_column(row):
    return jnp.transpose(jnp.broadcast_to(row, (128, row.shape[1])))


def layer_kernel(
    size,
    cap,
    tile,
    tok_hbm,
    latent_ref,
    clip_ref,
    expert_ref,
    slot_ref,
    gain1_ref,
    gain2_ref,
    router_ref,
    qkv_hbm,
    proj_hbm,
    w_in_hbm,
    w_out_hbm,
    out_ref,
    mean_ref,
    rows_ref,
    normed,
    w_qkv,
    w_proj,
    w_in,
    w_out,
    kv,
    queries,
    attended,
    bias,
    mid,
    expert_in,
    gates,
    places,
    sorted_place,
    buf,
    recv,
    res,
    back,
    acc,
    act,
    my_latent,
    peer_latent,
    tok_sem,
    qkv_sems,
    w_sems,
    lat_sems,
    send_sems,
    recv_sems,
    back_send,
    back_recv,
):
    near = NEAR if size % NEAR == 0 else 1
    far = size // near
    me = lax.axis_index("exp")
    mod = lax.axis_index("mod")
    high, low = me // near, me % near
    shifts = [0] + sorted(range(1, far), key=lambda s: (abs(2 * s - far), s))
    order = [(s, d) for s in shifts for d in range(near)]

    def ahead(step):
        s, d = order[step]
        return ((high + s) % far) * near + (low + d) % near

    def behind(step):
        s, d = order[step]
        return ((high + far - s) % far) * near + (low + near - d) % near

    def slots_of(step):
        return pl.ds(step * cap, cap)

    tokens = tok_hbm.shape[0]
    clips, per_clip, width = latent_ref.shape
    latents = clips * per_clip
    row_count = tokens + latents
    key_count = kv.shape[0]
    slot_total = size * cap

    load_tok = pltpu.make_async_copy(tok_hbm, rows_ref.at[pl.ds(0, tokens)], tok_sem)
    load_tok.start()
    loads = []
    for index in (1, 2, 0):
        cols = pl.ds(index * width, width)
        loads.append(
            pltpu.make_async_copy(qkv_hbm.at[:, cols], w_qkv.at[:, cols], qkv_sems.at[index])
        )
        loads[-1].start()
    load_k, load_v, load_q = loads
    load_proj = pltpu.make_async_copy(proj_hbm, w_proj, w_sems.at[2])
    load_in = pltpu.make_async_copy(w_in_hbm, w_in, w_sems.at[0])
    load_out = pltpu.make_async_copy(w_out_hbm, w_out, w_sems.at[1])
    load_proj.start()

    barrier = pltpu.get_barrier_semaphore()
    for step in range(1, size):
        pl.semaphore_signal(barrier, inc=1, device_id=(mod, ahead(step)), device_id_type=MESH)
    pl.semaphore_signal(barrier, inc=1, device_id=(1 - mod, me), device_id_type=MESH)

    sends = [None]
    backs = [None]
    for step in range(1, size):
        sends.append(
            pltpu.make_async_remote_copy(
                src_ref=buf.at[slots_of(step)],
                dst_ref=recv.at[slots_of(step)],
                send_sem=send_sems.at[step],
                recv_sem=recv_sems.at[step],
                device_id=(mod, ahead(step)),
                device_id_type=MESH,
            )
        )
        backs.append(
            pltpu.make_async_remote_copy(
                src_ref=res.at[slots_of(step)],
                dst_ref=back.at[slots_of(step)],
                send_sem=back_send.at[step],
                recv_sem=back_recv.at[step],
                device_id=(mod, behind(step)),
                device_id_type=MESH,
            )
        )

    experts = expert_ref[...]
    slots = slot_ref[...]
    served = slots < cap
    walk = list(range(near, size)) + list(range(near))
    steps = jnp.zeros_like(experts)
    rank = jnp.zeros_like(experts)
    start = jnp.zeros((1, 1), jnp.int32)
    lost = jnp.zeros((1, 1), jnp.int32)
    lost_rank = jnp.zeros_like(experts)
    for step in walk:
        here = experts == ahead(step)
        steps = jnp.where(here, step, steps)
        rank = jnp.where(here, start + slots, rank)
        lost_rank = jnp.where(here, lost + slots - cap, lost_rank)
        count = jnp.sum(jnp.where(here, 1.0, 0.0), axis=1, keepdims=True).astype(jnp.int32)
        start = start + jnp.minimum(count, cap)
        lost = lost + jnp.maximum(count - cap, 0)
    rank = jnp.where(served, rank, start + lost_rank)
    place_row = jnp.where(served, steps * cap + slots, slot_total)

    lane = lax.broadcasted_iota(jnp.int32, (1, key_count - tokens), 1)
    latent_clip = jnp.where(lane < latents, lane // per_clip, -1)
    token_clip = clip_ref[...] - me * clips
    clip_row = jnp.concatenate([token_clip, latent_clip], axis=1).astype(jnp.float32)

    field = lax.broadcasted_iota(jnp.int32, (16, tokens), 0)
    facts = jnp.where(
        field == 0,
        jnp.where(served, steps, size),
        jnp.where(field == 1, jnp.where(served, slots, 0), 0),
    ).astype(jnp.float32).astype(jnp.bfloat16)

    gain1 = gain1_ref[...].astype(jnp.float32)
    gain2 = gain2_ref[...].astype(jnp.float32)
    kv[pl.ds(row_count, key_count - row_count), :] = jnp.zeros(
        (key_count - row_count, kv.shape[1]), jnp.bfloat16
    )
    rows_ref[pl.ds(tokens, latents), :] = jnp.concatenate(
        [latent_ref[clip].astype(jnp.float32) for clip in range(clips)], axis=0
    ).astype(jnp.bfloat16)
    load_tok.wait()
    chunk = 48

    def norm1(i, carry):
        here = pl.ds(pl.multiple_of(i * chunk, 16), chunk)
        normed[here, :] = layer_norm(rows_ref[here, :].astype(jnp.float32), gain1).astype(
            jnp.bfloat16
        )
        return carry

    lax.fori_loop(0, row_count // chunk, norm1, 0)

    step_cols = 256

    def project_kv(load, offset):
        load.wait()

        def body(i, carry):
            src = pl.ds(pl.multiple_of(width + offset + i * step_cols, 128), step_cols)
            dst = pl.ds(pl.multiple_of(offset + i * step_cols, 128), step_cols)
            kv[pl.ds(0, row_count), dst] = matmul(normed[...], w_qkv[:, src]).astype(jnp.bfloat16)
            return carry

        lax.fori_loop(0, width // step_cols, body, 0)

    project_kv(load_k, 0)
    project_kv(load_v, width)

    pair = 128 // HEAD

    def attend(here, rows):
        def body(i, carry):
            for sub in range(PAIRS):
                p = i * PAIRS + sub
                cols = pl.ds(pl.multiple_of(p * 128, 128), 128)
                v_cols = pl.ds(pl.multiple_of(width + p * 128, 128), 128)
                key_block = kv[:, cols]
                value_block = kv[:, v_cols]
                query_block = queries[here, cols]
                head_of = lax.broadcasted_iota(jnp.int32, query_block.shape, 1) // HEAD
                total = jnp.zeros(query_block.shape, jnp.float32)
                for head in range(pair):
                    mine = head_of == head
                    scores = lax.dot_general(
                        jnp.where(mine, query_block, jnp.zeros_like(query_block)),
                        key_block,
                        (((1,), (1,)), ((), ())),
                        preferred_element_type=jnp.float32,
                    )
                    scores = scores + bias[here, :]
                    weights = jnp.exp(scores - jnp.max(scores, axis=-1, keepdims=True))
                    norm = jnp.sum(weights, axis=-1, keepdims=True)
                    summed = matmul(weights.astype(jnp.bfloat16), value_block)
                    total = jnp.where(mine, summed / norm, total)
                attended[here, cols] = total.astype(jnp.bfloat16)
            return carry

        lax.fori_loop(0, width // 128 // PAIRS, body, 0)

    inverse_root = jnp.bfloat16(1.0 / math.sqrt(HEAD))

    def project_q(first, rows):
        here = pl.ds(first, rows)

        def body(i, carry):
            cols = pl.ds(pl.multiple_of(i * step_cols, 128), step_cols)
            queries[here, cols] = (
                matmul(attended[here, :], w_qkv[:, cols]).astype(jnp.bfloat16) * inverse_root
            )
            return carry

        lax.fori_loop(0, width // step_cols, body, 0)

    row_in = lax.broadcasted_iota(jnp.int32, (EARLY, 1), 0)

    def gather(piece):
        here = pl.ds(piece * EARLY, EARLY)
        chosen = (piece * EARLY + row_in) == rank
        pick = one_hot(chosen)
        clip = jnp.sum(jnp.where(chosen, clip_row[:, :tokens], 0.0), axis=1, keepdims=True)
        bias[here, :] = jnp.where(clip == clip_row, 0.0, -jnp.inf)
        moved = lax.dot_general(
            facts, pick, (((1,), (1,)), ((), ())), preferred_element_type=jnp.float32
        ).astype(jnp.int32)
        at = moved[0:1, :] * cap + moved[1:2, :]
        sorted_place[:, here] = at
        attended[here, :] = matmul(pick, normed[pl.ds(0, tokens), :]).astype(jnp.bfloat16)
        acc[here, :] = matmul(pick, rows_ref[pl.ds(0, tokens), :])

    slot_row = lax.broadcasted_iota(jnp.int32, (128, 1), 0)

    def finish(piece):
        here = pl.ds(piece * EARLY, EARLY)
        attend(here, EARLY)
        if piece == 0:
            load_proj.wait()

        def project_out(i, carry):
            cols = pl.ds(pl.multiple_of(i * step_cols, 128), step_cols)
            acc[here, cols] += matmul(attended[here, :], w_proj[:, cols])
            return carry

        lax.fori_loop(0, width // step_cols, project_out, 0)
        half = EARLY // 2
        for part in range(2):
            some = pl.ds(piece * EARLY + part * half, half)
            expert_in[some, :] = layer_norm(acc[some, :], gain2).astype(jnp.bfloat16)

    def dispatch(base, count, known):
        pick = one_hot((base + slot_row[:count]) == sorted_place[:, pl.ds(0, known)])
        buf[pl.ds(base, count), :] = matmul(pick, expert_in[pl.ds(0, known), :]).astype(
            jnp.bfloat16
        )
        for step in range(base // cap, (base + count) // cap):
            if step:
                sends[step].start()
            else:
                recv[slots_of(0), :] = buf[slots_of(0), :]

    pieces = tokens // EARLY
    load_q.wait()
    gather(0)
    project_q(0, EARLY)
    finish(0)
    pl.semaphore_wait(barrier, size)
    base = near * cap
    dispatch(base, 128, EARLY)
    load_in.start()
    load_out.start()
    for piece in range(1, pieces):
        gather(piece)
    attended[pl.ds(tokens, latents), :] = normed[pl.ds(tokens, latents), :]
    project_q(EARLY, row_count - EARLY)
    for piece in range(1, pieces - 1):
        finish(piece)
        base += 128
        dispatch(base, 128, (piece + 1) * EARLY)
    finish(pieces - 1)
    for base in list(range(base + 128, slot_total, 128)) + list(range(0, near * cap, 128)):
        count = min(128, slot_total - base, near * cap - base if base < near * cap else 128)
        dispatch(base, count, tokens)

    tail = pl.ds(tokens, latents)
    tail_clip = lax.broadcasted_iota(jnp.int32, (latents, 1), 0) // per_clip
    bias[tail, :] = jnp.where(tail_clip.astype(jnp.float32) == clip_row, 0.0, -jnp.inf)
    attend(tail, latents)
    my_latent[...] = rows_ref[tail, :].astype(jnp.float32) + matmul(attended[tail, :], w_proj[...])
    latent_copy = pltpu.make_async_remote_copy(
        src_ref=my_latent,
        dst_ref=peer_latent,
        send_sem=lat_sems.at[0],
        recv_sem=lat_sems.at[1],
        device_id=(1 - mod, me),
        device_id_type=MESH,
    )
    latent_copy.start()

    logits = lax.dot_general(
        expert_in[...],
        router_ref[...],
        (((1,), (1,)), ((), ())),
        preferred_element_type=jnp.float32,
    )
    rank_col = to_column(rank.astype(jnp.float32)).astype(jnp.int32)
    places[...] = to_column(place_row.astype(jnp.float32)).astype(jnp.int32)
    expert_col = to_column(experts.astype(jnp.float32)).astype(jnp.int32)
    column = lax.broadcasted_iota(jnp.int32, (EARLY, size), 1)
    sorted_row = lax.broadcasted_iota(jnp.int32, (1, tokens), 1)

    def split(value):
        top = value.astype(jnp.bfloat16)
        return top, value - top.astype(jnp.float32)

    high_logits, rest = split(logits)
    middle_logits, rest = split(rest)
    low_logits, _ = split(rest)
    for piece in range(pieces):
        here = pl.ds(piece * EARLY, EARLY)
        pick = one_hot(rank_col[piece * EARLY : (piece + 1) * EARLY, 0:1] == sorted_row)
        own = (matmul(pick, high_logits) + matmul(pick, middle_logits)) + matmul(pick, low_logits)
        mine = column == expert_col[piece * EARLY : (piece + 1) * EARLY, 0:1]
        picked = jnp.sum(jnp.where(mine, own, 0.0), axis=1, keepdims=True)
        gates[here, :] = jnp.broadcast_to(jax.nn.sigmoid(picked), (EARLY, 128))

        def restore(i, carry):
            cols = pl.ds(pl.multiple_of(i * step_cols, 128), step_cols)
            first, rest = split(acc[:, cols])
            second, rest = split(rest)
            third, _ = split(rest)
            mid[here, cols] = (matmul(pick, first) + matmul(pick, second)) + matmul(pick, third)
            return carry

        lax.fori_loop(0, width // step_cols, restore, 0)

    groups = 2 if size % 4 == 0 else 1
    steps_per = size // groups
    group_rows = steps_per * cap
    tiles = w_in.shape[1] // tile
    for g in range(groups):
        for step in range(g * steps_per, (g + 1) * steps_per):
            if step:
                sends[step].wait_recv()
        if g == 0:
            load_in.wait()
            load_out.wait()
        here = pl.ds(g * group_rows, group_rows)

        def hidden(t):
            cols = pl.ds(pl.multiple_of(t * tile, tile), tile)
            return gelu(matmul(recv[here, :], w_in[:, cols])).astype(jnp.bfloat16)

        def project(t, slot):
            cols = pl.ds(pl.multiple_of(t * tile, tile), tile)
            return matmul(act[slot], w_out[cols, :])

        act[0] = hidden(0)
        acc[...] = jnp.zeros_like(acc)

        def body(t, carry):
            acc[...] += project(t - 1, (t + 1) % 2)
            act[t % 2] = hidden(t)
            return carry

        lax.fori_loop(1, tiles, body, 0)
        res[here, :] = (acc[...] + project(tiles - 1, (tiles - 1) % 2)).astype(jnp.bfloat16)
        for step in range(g * steps_per, (g + 1) * steps_per):
            if step:
                backs[step].start()
            else:
                back[slots_of(0), :] = res[slots_of(0), :]

    latent_copy.wait()
    mean = (my_latent[...] + peer_latent[...]) * 0.5
    for clip in range(clips):
        mean_ref[clip] = mean[clip * per_clip : (clip + 1) * per_clip, :].astype(jnp.bfloat16)

    for g in range(groups):
        for step in range(g * steps_per, (g + 1) * steps_per):
            if step:
                backs[step].wait_recv()

        def combine(i, carry):
            here = pl.ds(pl.multiple_of(i * 128, 128), 128)
            slot = lax.broadcasted_iota(jnp.int32, (1, group_rows), 1) + g * group_rows
            pick = one_hot(places[here, 0:1] == slot)
            returned = matmul(pick, back[pl.ds(g * group_rows, group_rows), :])
            mixed = mid[here, :] + gates[here, 0:1] * returned
            if g == groups - 1:
                out_ref[here, :] = mixed.astype(jnp.bfloat16)
            else:
                mid[here, :] = mixed
            return carry

        lax.fori_loop(0, tokens // 128, combine, 0)
    for step in range(1, size):
        sends[step].wait_send()
        backs[step].wait_send()


def layer(
    tokens, bottleneck, clip, expert, slot, gain1, gain2, router, w_qkv, w_proj, w_in, w_out, size
):
    count, width = tokens.shape
    latents = bottleneck.shape[0] * bottleneck.shape[1]
    hidden_width = w_in.shape[1]
    rows = count + latents
    keys = count + 128
    cap = CAP_FACTOR * count // size
    slots = size * cap
    groups = 2 if size % 4 == 0 else 1
    tile = 1024
    vmem = pl.BlockSpec(memory_space=pltpu.VMEM)
    hbm = pl.BlockSpec(memory_space=pl.ANY)
    bf16, f32 = jnp.bfloat16, jnp.float32
    dma = pltpu.SemaphoreType.DMA
    return pl.pallas_call(
        functools.partial(layer_kernel, size, cap, tile),
        out_shape=(
            jax.ShapeDtypeStruct((count, width), bf16),
            jax.ShapeDtypeStruct(bottleneck.shape, bf16),
        ),
        in_specs=[hbm] + [vmem] * 7 + [hbm] * 4,
        out_specs=(vmem, vmem),
        scratch_shapes=[
            pltpu.VMEM((rows, width), bf16),
            pltpu.VMEM((rows, width), bf16),
            pltpu.VMEM((width, 3 * width), bf16),
            pltpu.VMEM((width, width), bf16),
            pltpu.VMEM((width, hidden_width), bf16),
            pltpu.VMEM((hidden_width, width), bf16),
            pltpu.VMEM((keys, 2 * width), bf16),
            pltpu.VMEM((rows, width), bf16),
            pltpu.VMEM((rows, width), bf16),
            pltpu.VMEM((rows, keys), f32),
            pltpu.VMEM((count, width), f32),
            pltpu.VMEM((count, width), bf16),
            pltpu.VMEM((count, 128), f32),
            pltpu.VMEM((count, 128), jnp.int32),
            pltpu.VMEM((1, count), jnp.int32),
            pltpu.VMEM((slots, width), bf16),
            pltpu.VMEM((slots, width), bf16),
            pltpu.VMEM((slots, width), bf16),
            pltpu.VMEM((slots, width), bf16),
            pltpu.VMEM((slots // groups, width), f32),
            pltpu.VMEM((2, slots // groups, tile), bf16),
            pltpu.VMEM((latents, width), f32),
            pltpu.VMEM((latents, width), f32),
            dma(()),
            dma((3,)),
            dma((3,)),
            dma((2,)),
            dma((size,)),
            dma((size,)),
            dma((size,)),
            dma((size,)),
        ],
        compiler_params=pltpu.CompilerParams(
            collective_id=0, has_side_effects=True, vmem_limit_bytes=56 * 1024 * 1024
        ),
    )(tokens, bottleneck, clip, expert, slot, gain1, gain2, router, w_qkv, w_proj, w_in, w_out)


def on_device(
    size,
    tokens,
    bottleneck,
    clip_ids,
    expert_ids,
    slots,
    norm1_gain,
    attn_qkv,
    attn_out,
    norm2_gain,
    router,
    fc_in,
    fc_out,
):
    mixed, latent = layer(
        tokens[0],
        bottleneck,
        clip_ids,
        expert_ids,
        slots,
        norm1_gain,
        norm2_gain,
        router.T,
        attn_qkv[0],
        attn_out[0],
        fc_in[0],
        fc_out[0],
        size,
    )
    return (mixed[None], latent)


def solution(mesh):
    in_specs = (
        P("mod", "exp", None),
        P("exp", None, None),
        P("mod", "exp"),
        P("mod", "exp"),
        P("mod", "exp"),
        P("mod", None),
        P("mod", None, None),
        P("mod", None, None),
        P("mod", None),
        P(),
        P("exp", None, None),
        P("exp", None, None),
    )
    out_specs = (P("mod", "exp", None), P("exp", None, None))
    return jax.shard_map(
        functools.partial(on_device, mesh.shape["exp"]),
        mesh=mesh,
        in_specs=in_specs,
        out_specs=out_specs,
        check_vma=False,
    )
```

```python
import functools
import math

import jax
import jax.numpy as jnp
from jax import lax
from jax.experimental import pallas as pl
from jax.experimental.pallas import tpu as pltpu
from jax.sharding import PartitionSpec as P

MESH = pl.DeviceIdType.MESH
HEAD = 64
CAP_FACTOR = 2
EARLY = 128
FEW = 64
PAIRS = 2
NEAR = 4


EPSILON = 1e-06


def layer_norm(features, scales):
    row_mean = jnp.mean(features, axis=-1, keepdims=True)
    centred = features - row_mean
    spread = jnp.mean(centred * centred, axis=-1, keepdims=True)
    return centred * lax.rsqrt(spread + EPSILON) * scales


def gelu(x):
    half = 0.5 * x
    return half + half * lax.erf(x * (1.0 / math.sqrt(2.0)))


def matmul(lhs, rhs):
    return jnp.dot(lhs, rhs, preferred_element_type=jnp.float32)


def one_hot(condition):
    return jnp.where(condition, 1.0, 0.0).astype(jnp.bfloat16)


def to_column(row):
    return jnp.transpose(jnp.broadcast_to(row, (128, row.shape[1])))


def layer_kernel(
    size,
    cap,
    tile,
    tok_hbm,
    latent_hbm,
    clip_hbm,
    expert_hbm,
    slot_hbm,
    gain1_hbm,
    gain2_hbm,
    router_hbm,
    qkv_hbm,
    proj_hbm,
    w_in_hbm,
    w_out_hbm,
    out_ref,
    mean_ref,
    latent_ref,
    clip_ref,
    expert_ref,
    slot_ref,
    gain1_ref,
    gain2_ref,
    router_ref,
    rows_ref,
    normed,
    w_qkv,
    w_proj,
    w_in,
    w_out,
    key_ref,
    value_t,
    key_clips,
    queries,
    attended,
    bias,
    mid,
    expert_in,
    gates,
    places,
    sorted_place,
    row_clips,
    buf,
    recv,
    res,
    back,
    acc,
    act,
    sums,
    my_latent,
    peer_latent,
    tok_sem,
    small_sems,
    qkv_sems,
    w_sems,
    lat_sems,
    send_sems,
    recv_sems,
    back_send,
    back_recv,
):
    near = NEAR if size % NEAR == 0 else 1
    far = size // near
    me = lax.axis_index("exp")
    mod = lax.axis_index("mod")
    high, low = me // near, me % near
    shifts = [0] + sorted(range(1, far), key=lambda s: (abs(2 * s - far), s))
    order = [(s, d) for s in shifts for d in range(near)]

    def ahead(step):
        s, d = order[step]
        return ((high + s) % far) * near + (low + d) % near

    def behind(step):
        s, d = order[step]
        return ((high + far - s) % far) * near + (low + near - d) % near

    def slots_of(step):
        return pl.ds(step * cap, cap)

    tokens = tok_hbm.shape[0]
    clips, per_clip, width = latent_ref.shape
    latents = clips * per_clip
    row_count = tokens + latents
    key_count = key_ref.shape[0]
    slot_total = size * cap

    load_tok = pltpu.make_async_copy(tok_hbm, rows_ref.at[pl.ds(0, tokens)], tok_sem)
    load_tok.start()
    small = [
        pltpu.make_async_copy(src, dst, small_sems.at[index])
        for index, (src, dst) in enumerate(
            (
                (expert_hbm, expert_ref),
                (slot_hbm, slot_ref),
                (clip_hbm, clip_ref),
                (gain1_hbm, gain1_ref),
                (latent_hbm, latent_ref),
                (gain2_hbm, gain2_ref),
                (router_hbm, router_ref),
            )
        )
    ]
    for copy in small:
        copy.start()
    loads = []
    for index in (1, 2, 0):
        cols = pl.ds(index * width, width)
        loads.append(
            pltpu.make_async_copy(qkv_hbm.at[:, cols], w_qkv.at[:, cols], qkv_sems.at[index])
        )
    load_k, load_v, load_q = loads
    load_k.start()
    load_proj = pltpu.make_async_copy(proj_hbm, w_proj, w_sems.at[2])
    load_in = pltpu.make_async_copy(w_in_hbm, w_in, w_sems.at[0])
    load_out = pltpu.make_async_copy(w_out_hbm, w_out, w_sems.at[1])

    barrier = pltpu.get_barrier_semaphore()
    for step in range(1, size):
        pl.semaphore_signal(barrier, inc=1, device_id=(mod, ahead(step)), device_id_type=MESH)
    pl.semaphore_signal(barrier, inc=1, device_id=(1 - mod, me), device_id_type=MESH)

    sends = [None]
    backs = [None]
    for step in range(1, size):
        sends.append(
            pltpu.make_async_remote_copy(
                src_ref=buf.at[slots_of(step)],
                dst_ref=recv.at[slots_of(step)],
                send_sem=send_sems.at[step],
                recv_sem=recv_sems.at[step],
                device_id=(mod, ahead(step)),
                device_id_type=MESH,
            )
        )
        backs.append(
            pltpu.make_async_remote_copy(
                src_ref=res.at[slots_of(step)],
                dst_ref=back.at[slots_of(step)],
                send_sem=back_send.at[step],
                recv_sem=back_recv.at[step],
                device_id=(mod, behind(step)),
                device_id_type=MESH,
            )
        )

    for copy in small:
        copy.wait()
    experts = expert_ref[...]
    slots = slot_ref[...]
    served = slots < cap
    walk = list(range(near, size)) + list(range(near))
    steps = jnp.zeros_like(experts)
    rank = jnp.zeros_like(experts)
    start = jnp.zeros((1, 1), jnp.int32)
    lost = jnp.zeros((1, 1), jnp.int32)
    lost_rank = jnp.zeros_like(experts)
    for step in walk:
        here = experts == ahead(step)
        steps = jnp.where(here, step, steps)
        rank = jnp.where(here, start + slots, rank)
        lost_rank = jnp.where(here, lost + slots - cap, lost_rank)
        count = jnp.sum(jnp.where(here, 1.0, 0.0), axis=1, keepdims=True).astype(jnp.int32)
        start = start + jnp.minimum(count, cap)
        lost = lost + jnp.maximum(count - cap, 0)
    rank = jnp.where(served, rank, start + lost_rank)
    place_row = jnp.where(served, steps * cap + slots, slot_total)

    lane = lax.broadcasted_iota(jnp.int32, (1, key_count - tokens), 1)
    latent_clip = jnp.where(lane < latents, lane // per_clip, -1)
    token_clip = clip_ref[...] - me * clips
    clip_row = jnp.concatenate([token_clip, latent_clip], axis=1).astype(jnp.float32)

    field = lax.broadcasted_iota(jnp.int32, (16, tokens), 0)
    facts = jnp.where(
        field == 0,
        jnp.where(served, steps, size),
        jnp.where(
            field == 1, jnp.where(served, slots, 0), jnp.where(field == 2, token_clip, 0)
        ),
    ).astype(jnp.float32).astype(jnp.bfloat16)

    gain1 = gain1_ref[...].astype(jnp.float32)
    gain2 = gain2_ref[...].astype(jnp.float32)
    key_clips[...] = to_column(clip_row)
    padding = key_count - row_count
    key_ref[pl.ds(row_count, padding), :] = jnp.zeros((padding, width), jnp.bfloat16)
    rows_ref[pl.ds(tokens, latents), :] = jnp.concatenate(
        [latent_ref[clip].astype(jnp.float32) for clip in range(clips)], axis=0
    ).astype(jnp.bfloat16)
    load_tok.wait()
    load_v.start()
    load_q.start()
    load_proj.start()
    chunk = 48

    def norm1(i, carry):
        here = pl.ds(pl.multiple_of(i * chunk, 16), chunk)
        normed[here, :] = layer_norm(rows_ref[here, :].astype(jnp.float32), gain1).astype(
            jnp.bfloat16
        )
        return carry

    lax.fori_loop(0, row_count // chunk, norm1, 0)

    step_cols = 256

    def project_key(i, carry):
        src = pl.ds(pl.multiple_of(width + i * step_cols, 128), step_cols)
        dst = pl.ds(pl.multiple_of(i * step_cols, 128), step_cols)
        key_ref[pl.ds(0, row_count), dst] = matmul(normed[...], w_qkv[:, src]).astype(jnp.bfloat16)
        return carry

    def project_value(i, carry):
        src = pl.ds(pl.multiple_of(2 * width + i * step_cols, 128), step_cols)
        dst = pl.ds(pl.multiple_of(i * step_cols, 128), step_cols)
        block = matmul(normed[...], w_qkv[:, src]).astype(jnp.bfloat16)
        zeros = jnp.zeros((padding, step_cols), jnp.bfloat16)
        value_t[dst, :] = jnp.transpose(jnp.concatenate([block, zeros], axis=0))
        return carry

    load_k.wait()
    lax.fori_loop(0, width // step_cols, project_key, 0)
    load_v.wait()
    lax.fori_loop(0, width // step_cols, project_value, 0)

    pair = 128 // HEAD

    def attend_few(first):
        here = pl.ds(first, FEW)
        wide = 2 * 128

        def body(i, carry):
            for sub in range(PAIRS):
                at = (i * PAIRS + sub) * wide
                cols = pl.ds(pl.multiple_of(at, 128), wide)
                block = queries[here, cols]
                head_of = lax.broadcasted_iota(jnp.int32, block.shape, 1) // HEAD
                stacked = jnp.concatenate(
                    [
                        jnp.where(head_of == head, block, jnp.zeros_like(block))
                        for head in range(wide // HEAD)
                    ],
                    axis=0,
                )
                scores = lax.dot_general(
                    key_ref[:, cols],
                    stacked,
                    (((1,), (1,)), ((), ())),
                    preferred_element_type=jnp.float32,
                )
                scores = scores + jnp.concatenate([bias[...]] * 2, axis=1)
                weights = jnp.exp(scores - jnp.max(scores, axis=0, keepdims=True))
                norm = jnp.sum(weights, axis=0, keepdims=True)
                summed = matmul(value_t[cols, :], weights.astype(jnp.bfloat16))
                lane_of = lax.broadcasted_iota(jnp.int32, (FEW, 128), 1)
                for j in range(2):
                    part = slice(j * 128, (j + 1) * 128)
                    turned = jnp.transpose(summed[part, part] / norm[:, part])
                    both = jnp.where(lane_of < HEAD, turned[:FEW], turned[FEW:])
                    dst = pl.ds(pl.multiple_of(at + j * 128, 128), 128)
                    attended[here, dst] = both.astype(jnp.bfloat16)
            return carry

        lax.fori_loop(0, width // wide // PAIRS, body, 0)

    def attend(first):
        here = pl.ds(first, EARLY)

        def body(i, carry):
            for sub in range(PAIRS):
                cols = pl.ds(pl.multiple_of((i * PAIRS + sub) * 128, 128), 128)
                block = queries[here, cols]
                head_of = lax.broadcasted_iota(jnp.int32, block.shape, 1) // HEAD
                stacked = jnp.concatenate(
                    [jnp.where(head_of == head, block, jnp.zeros_like(block)) for head in range(pair)],
                    axis=0,
                )
                scores = lax.dot_general(
                    key_ref[:, cols],
                    stacked,
                    (((1,), (1,)), ((), ())),
                    preferred_element_type=jnp.float32,
                )
                scores = scores + jnp.concatenate([bias[...]] * pair, axis=1)
                weights = jnp.exp(scores - jnp.max(scores, axis=0, keepdims=True))
                norm = jnp.sum(weights, axis=0, keepdims=True)
                summed = matmul(value_t[cols, :], weights.astype(jnp.bfloat16))
                heads = [
                    summed[head * HEAD : (head + 1) * HEAD, head * EARLY : (head + 1) * EARLY]
                    / norm[:, head * EARLY : (head + 1) * EARLY]
                    for head in range(pair)
                ]
                attended[here, cols] = jnp.transpose(jnp.concatenate(heads, axis=0)).astype(
                    jnp.bfloat16
                )
            return carry

        lax.fori_loop(0, width // 128 // PAIRS, body, 0)

    inverse_root = jnp.bfloat16(1.0 / math.sqrt(HEAD))

    def project_q(first, rows):
        here = pl.ds(first, rows)

        def body(i, carry):
            cols = pl.ds(pl.multiple_of(i * step_cols, 128), step_cols)
            queries[here, cols] = (
                matmul(attended[here, :], w_qkv[:, cols]).astype(jnp.bfloat16) * inverse_root
            )
            return carry

        lax.fori_loop(0, width // step_cols, body, 0)

    row_in = lax.broadcasted_iota(jnp.int32, (EARLY, 1), 0)

    def gather(first, rows):
        here = pl.ds(first, rows)
        chosen = (first + row_in[:rows]) == rank
        pick = one_hot(chosen)
        moved = lax.dot_general(
            facts, pick, (((1,), (1,)), ((), ())), preferred_element_type=jnp.float32
        )
        row_clips[:, here] = moved[2:3, :]
        moved = moved.astype(jnp.int32)
        at = moved[0:1, :] * cap + moved[1:2, :]
        sorted_place[:, here] = at
        attended[here, :] = matmul(pick, normed[pl.ds(0, tokens), :]).astype(jnp.bfloat16)
        sums[here, :] = matmul(pick, rows_ref[pl.ds(0, tokens), :])

    slot_row = lax.broadcasted_iota(jnp.int32, (128, 1), 0)

    def mask(clips_across):
        bias[...] = jnp.where(key_clips[...] == clips_across, 0.0, -jnp.inf)

    def finish(first, rows):
        here = pl.ds(first, rows)
        if rows == FEW:
            mask(jnp.concatenate([row_clips[:, here]] * 2, axis=1))
            attend_few(first)
        else:
            mask(row_clips[:, here])
            attend(first)
        if first == 0:
            load_proj.wait()

        def project_out(i, carry):
            cols = pl.ds(pl.multiple_of(i * step_cols, 128), step_cols)
            sums[here, cols] += matmul(attended[here, :], w_proj[:, cols])
            return carry

        lax.fori_loop(0, width // step_cols, project_out, 0)
        half = rows // 2
        for part in range(2):
            some = pl.ds(first + part * half, half)
            expert_in[some, :] = layer_norm(sums[some, :], gain2).astype(jnp.bfloat16)

    def dispatch(base, count, known):
        pick = one_hot((base + slot_row[:count]) == sorted_place[:, pl.ds(0, known)])
        buf[pl.ds(base, count), :] = matmul(pick, expert_in[pl.ds(0, known), :]).astype(
            jnp.bfloat16
        )
        for step in range(base // cap, (base + count) // cap):
            if step:
                sends[step].start()
            else:
                recv[slots_of(0), :] = buf[slots_of(0), :]

    pieces = tokens // EARLY
    parts = [(0, FEW), (FEW, FEW)] + [(piece * EARLY, EARLY) for piece in range(1, pieces)]
    load_q.wait()
    gather(0, FEW)
    project_q(0, FEW)
    finish(0, FEW)
    pl.semaphore_wait(barrier, size)
    base = near * cap
    dispatch(base, FEW, FEW)
    load_in.start()
    load_out.start()
    gather(FEW, FEW)
    project_q(FEW, FEW)
    finish(FEW, FEW)
    dispatch(base + FEW, FEW, 2 * FEW)
    gather(EARLY, EARLY)
    project_q(EARLY, EARLY)
    finish(EARLY, EARLY)
    dispatch(base + EARLY, EARLY, 2 * EARLY)
    for first, rows in parts[3:]:
        gather(first, rows)
    attended[pl.ds(tokens, latents), :] = normed[pl.ds(tokens, latents), :]
    attended[pl.ds(row_count, padding), :] = jnp.zeros((padding, width), jnp.bfloat16)
    project_q(2 * EARLY, key_count - 2 * EARLY)
    for first, rows in parts[3:-1]:
        finish(first, rows)
        dispatch(base + first, rows, first + rows)
    finish(*parts[-1])
    base += parts[-1][0]
    for base in list(range(base, slot_total, 128)) + list(range(0, near * cap, 128)):
        count = min(128, slot_total - base, near * cap - base if base < near * cap else 128)
        dispatch(base, count, tokens)

    groups = 4 if size % 4 == 0 else 1
    steps_per = size // groups
    group_rows = steps_per * cap
    tiles = w_in.shape[1] // tile
    for turn, g in enumerate([1, 0, 2, 3] if groups == 4 else [0]):
        for step in range(g * steps_per, (g + 1) * steps_per):
            if step:
                sends[step].wait_recv()
        if turn == 0:
            load_in.wait()
            load_out.wait()
        here = pl.ds(g * group_rows, group_rows)

        def hidden(t):
            cols = pl.ds(pl.multiple_of(t * tile, tile), tile)
            return gelu(matmul(recv[here, :], w_in[:, cols])).astype(jnp.bfloat16)

        def project(t, slot):
            cols = pl.ds(pl.multiple_of(t * tile, tile), tile)
            return matmul(act[slot], w_out[cols, :])

        act[0] = hidden(0)
        acc[...] = jnp.zeros_like(acc)

        def body(t, carry):
            acc[...] += project(t - 1, (t + 1) % 2)
            act[t % 2] = hidden(t)
            return carry

        lax.fori_loop(1, tiles, body, 0)
        res[here, :] = (acc[...] + project(tiles - 1, (tiles - 1) % 2)).astype(jnp.bfloat16)
        for step in range(g * steps_per, (g + 1) * steps_per):
            if step:
                backs[step].start()
            else:
                back[slots_of(0), :] = res[slots_of(0), :]

    tail = pl.ds(tokens, latents)
    mask(latent_clip.astype(jnp.float32))
    attend(tokens)
    my_latent[...] = rows_ref[tail, :].astype(jnp.float32) + matmul(attended[tail, :], w_proj[...])
    latent_copy = pltpu.make_async_remote_copy(
        src_ref=my_latent,
        dst_ref=peer_latent,
        send_sem=lat_sems.at[0],
        recv_sem=lat_sems.at[1],
        device_id=(1 - mod, me),
        device_id_type=MESH,
    )
    latent_copy.start()

    logits = lax.dot_general(
        expert_in[...],
        router_ref[...],
        (((1,), (1,)), ((), ())),
        preferred_element_type=jnp.float32,
    )
    rank_col = to_column(rank.astype(jnp.float32)).astype(jnp.int32)
    places[...] = to_column(place_row.astype(jnp.float32)).astype(jnp.int32)
    expert_col = to_column(experts.astype(jnp.float32)).astype(jnp.int32)
    column = lax.broadcasted_iota(jnp.int32, (EARLY, size), 1)
    sorted_row = lax.broadcasted_iota(jnp.int32, (1, tokens), 1)

    def split(value):
        top = value.astype(jnp.bfloat16)
        return top, value - top.astype(jnp.float32)

    high_logits, rest = split(logits)
    middle_logits, rest = split(rest)
    low_logits, _ = split(rest)
    for piece in range(pieces):
        here = pl.ds(piece * EARLY, EARLY)
        pick = one_hot(rank_col[piece * EARLY : (piece + 1) * EARLY, 0:1] == sorted_row)
        own = (matmul(pick, high_logits) + matmul(pick, middle_logits)) + matmul(pick, low_logits)
        mine = column == expert_col[piece * EARLY : (piece + 1) * EARLY, 0:1]
        picked = jnp.sum(jnp.where(mine, own, 0.0), axis=1, keepdims=True)
        gates[here, :] = jnp.broadcast_to(jax.nn.sigmoid(picked), (EARLY, 128))

        def restore(i, carry):
            cols = pl.ds(pl.multiple_of(i * step_cols, 128), step_cols)
            first, rest = split(sums[:, cols])
            second, rest = split(rest)
            third, _ = split(rest)
            mid[here, cols] = (matmul(pick, first) + matmul(pick, second)) + matmul(pick, third)
            return carry

        lax.fori_loop(0, width // step_cols, restore, 0)

    latent_copy.wait()
    mean = (my_latent[...] + peer_latent[...]) * 0.5
    for clip in range(clips):
        mean_ref[clip] = mean[clip * per_clip : (clip + 1) * per_clip, :].astype(jnp.bfloat16)

    cuts = [0, size // 2, size - size // 4, size] if size % 4 == 0 else [0, size]
    for first, last in zip(cuts[:-1], cuts[1:]):
        for step in range(first, last):
            if step:
                backs[step].wait_recv()
        some = pl.ds(first * cap, (last - first) * cap)

        def combine(i, carry):
            here = pl.ds(pl.multiple_of(i * 128, 128), 128)
            slot = lax.broadcasted_iota(jnp.int32, (1, (last - first) * cap), 1) + first * cap
            pick = one_hot(places[here, 0:1] == slot)
            mixed = mid[here, :] + gates[here, 0:1] * matmul(pick, back[some, :])
            if last == size:
                out_ref[here, :] = mixed.astype(jnp.bfloat16)
            else:
                mid[here, :] = mixed
            return carry

        lax.fori_loop(0, tokens // 128, combine, 0)
    for step in range(1, size):
        sends[step].wait_send()
        backs[step].wait_send()


def layer(
    tokens, bottleneck, clip, expert, slot, gain1, gain2, router, w_qkv, w_proj, w_in, w_out, size
):
    count, width = tokens.shape
    latents = bottleneck.shape[0] * bottleneck.shape[1]
    hidden_width = w_in.shape[1]
    rows = count + latents
    keys = count + 128
    cap = CAP_FACTOR * count // size
    slots = size * cap
    groups = 4 if size % 4 == 0 else 1
    tile = 1024
    vmem = pl.BlockSpec(memory_space=pltpu.VMEM)
    hbm = pl.BlockSpec(memory_space=pl.ANY)
    bf16, f32 = jnp.bfloat16, jnp.float32
    dma = pltpu.SemaphoreType.DMA
    return pl.pallas_call(
        functools.partial(layer_kernel, size, cap, tile),
        out_shape=(
            pltpu.VMEM((count, width), bf16),
            pltpu.VMEM(bottleneck.shape, bf16),
        ),
        in_specs=[hbm] * 12,
        out_specs=(vmem, vmem),
        scratch_shapes=[
            pltpu.VMEM(bottleneck.shape, bf16),
            pltpu.VMEM(clip.shape, jnp.int32),
            pltpu.VMEM(expert.shape, jnp.int32),
            pltpu.VMEM(slot.shape, jnp.int32),
            pltpu.VMEM(gain1.shape, bf16),
            pltpu.VMEM(gain2.shape, bf16),
            pltpu.VMEM(router.shape, bf16),
            pltpu.VMEM((rows, width), bf16),
            pltpu.VMEM((rows, width), bf16),
            pltpu.VMEM((width, 3 * width), bf16),
            pltpu.VMEM((width, width), bf16),
            pltpu.VMEM((width, hidden_width), bf16),
            pltpu.VMEM((hidden_width, width), bf16),
            pltpu.VMEM((keys, width), bf16),
            pltpu.VMEM((width, keys), bf16),
            pltpu.VMEM((keys, 128), f32),
            pltpu.VMEM((keys, width), bf16),
            pltpu.VMEM((keys, width), bf16),
            pltpu.VMEM((keys, EARLY), f32),
            pltpu.VMEM((count, width), f32),
            pltpu.VMEM((count, width), bf16),
            pltpu.VMEM((count, 128), f32),
            pltpu.VMEM((count, 128), jnp.int32),
            pltpu.VMEM((1, count), jnp.int32),
            pltpu.VMEM((1, count), f32),
            pltpu.VMEM((slots, width), bf16),
            pltpu.VMEM((slots, width), bf16),
            pltpu.VMEM((slots, width), bf16),
            pltpu.VMEM((slots, width), bf16),
            pltpu.VMEM((slots // groups, width), f32),
            pltpu.VMEM((2, slots // groups, tile), bf16),
            pltpu.VMEM((count, width), f32),
            pltpu.VMEM((latents, width), f32),
            pltpu.VMEM((latents, width), f32),
            dma(()),
            dma((7,)),
            dma((3,)),
            dma((3,)),
            dma((2,)),
            dma((size,)),
            dma((size,)),
            dma((size,)),
            dma((size,)),
        ],
        compiler_params=pltpu.CompilerParams(
            collective_id=0, has_side_effects=True, vmem_limit_bytes=56 * 1024 * 1024
        ),
    )(tokens, bottleneck, clip, expert, slot, gain1, gain2, router, w_qkv, w_proj, w_in, w_out)


def on_device(
    size,
    tokens,
    bottleneck,
    clip_ids,
    expert_ids,
    slots,
    norm1_gain,
    attn_qkv,
    attn_out,
    norm2_gain,
    router,
    fc_in,
    fc_out,
):
    mixed, latent = layer(
        tokens[0],
        bottleneck,
        clip_ids,
        expert_ids,
        slots,
        norm1_gain,
        norm2_gain,
        router.T,
        attn_qkv[0],
        attn_out[0],
        fc_in[0],
        fc_out[0],
        size,
    )
    return (mixed[None], latent)


def solution(mesh):
    in_specs = (
        P("mod", "exp", None),
        P("exp", None, None),
        P("mod", "exp"),
        P("mod", "exp"),
        P("mod", "exp"),
        P("mod", None),
        P("mod", None, None),
        P("mod", None, None),
        P("mod", None),
        P(),
        P("exp", None, None),
        P("exp", None, None),
    )
    out_specs = (P("mod", "exp", None), P("exp", None, None))
    return jax.shard_map(
        functools.partial(on_device, mesh.shape["exp"]),
        mesh=mesh,
        in_specs=in_specs,
        out_specs=out_specs,
        check_vma=False,
    )
```

```python
import functools
import math

import jax
import jax.numpy as jnp
from jax import lax
from jax.experimental import pallas as pl
from jax.experimental.pallas import tpu as pltpu
from jax.sharding import PartitionSpec as P

MESH = pl.DeviceIdType.MESH
HEAD = 64
CAP_FACTOR = 2
EARLY = 128
FEW = 64
PAIRS = 2
NEAR = 4


EPSILON = 1e-06


def layer_norm(features, scales):
    row_mean = jnp.mean(features, axis=-1, keepdims=True)
    centred = features - row_mean
    spread = jnp.mean(centred * centred, axis=-1, keepdims=True)
    return centred * lax.rsqrt(spread + EPSILON) * scales


def gelu(x):
    half = 0.5 * x
    return half + half * lax.erf(x * (1.0 / math.sqrt(2.0)))


def matmul(lhs, rhs):
    return jnp.dot(lhs, rhs, preferred_element_type=jnp.float32)


def one_hot(condition):
    return jnp.where(condition, 1.0, 0.0).astype(jnp.bfloat16)


def to_column(row):
    return jnp.transpose(jnp.broadcast_to(row, (128, row.shape[1])))


def layer_kernel(
    size,
    cap,
    tile,
    tok_hbm,
    latent_hbm,
    clip_hbm,
    expert_hbm,
    slot_hbm,
    gain1_hbm,
    gain2_hbm,
    router_hbm,
    qkv_hbm,
    proj_hbm,
    w_in_hbm,
    w_out_hbm,
    out_ref,
    mean_ref,
    latent_ref,
    clip_ref,
    expert_ref,
    slot_ref,
    gain1_ref,
    gain2_ref,
    router_ref,
    rows_ref,
    normed,
    w_qkv,
    w_proj,
    w_in,
    w_out,
    key_ref,
    value_t,
    key_clips,
    queries,
    attended,
    bias,
    mid,
    expert_in,
    gates,
    places,
    sorted_place,
    row_clips,
    buf,
    recv,
    res,
    back,
    acc,
    act,
    sums,
    my_latent,
    peer_latent,
    tok_sem,
    small_sems,
    qkv_sems,
    w_sems,
    lat_sems,
    send_sems,
    recv_sems,
    back_send,
    back_recv,
):
    near = NEAR if size % NEAR == 0 else 1
    far = size // near
    me = lax.axis_index("exp")
    mod = lax.axis_index("mod")
    high, low = me // near, me % near
    shifts = [0] + sorted(range(1, far), key=lambda s: (abs(2 * s - far), s))
    order = [(s, d) for s in shifts[:2] for d in range(near)]
    for index in range(2, far, 2):
        order += [(s, d) for d in range(near) for s in shifts[index : index + 2]]

    def ahead(step):
        s, d = order[step]
        return ((high + s) % far) * near + (low + d) % near

    def behind(step):
        s, d = order[step]
        return ((high + far - s) % far) * near + (low + near - d) % near

    def slots_of(step):
        return pl.ds(step * cap, cap)

    tokens = tok_hbm.shape[0]
    clips, per_clip, width = latent_ref.shape
    latents = clips * per_clip
    row_count = tokens + latents
    key_count = key_ref.shape[0]
    slot_total = size * cap

    load_tok = pltpu.make_async_copy(tok_hbm, rows_ref.at[pl.ds(0, tokens)], tok_sem)
    load_tok.start()
    small = [
        pltpu.make_async_copy(src, dst, small_sems.at[index])
        for index, (src, dst) in enumerate(
            (
                (expert_hbm, expert_ref),
                (slot_hbm, slot_ref),
                (clip_hbm, clip_ref),
                (gain1_hbm, gain1_ref),
                (latent_hbm, latent_ref),
                (gain2_hbm, gain2_ref),
                (router_hbm, router_ref),
            )
        )
    ]
    for copy in small:
        copy.start()
    loads = []
    for index in (1, 2, 0):
        cols = pl.ds(index * width, width)
        loads.append(
            pltpu.make_async_copy(qkv_hbm.at[:, cols], w_qkv.at[:, cols], qkv_sems.at[index])
        )
    load_k, load_v, load_q = loads
    load_k.start()
    load_proj = pltpu.make_async_copy(proj_hbm, w_proj, w_sems.at[2])
    load_in = pltpu.make_async_copy(w_in_hbm, w_in, w_sems.at[0])
    load_out = pltpu.make_async_copy(w_out_hbm, w_out, w_sems.at[1])

    barrier = pltpu.get_barrier_semaphore()
    for step in range(1, size):
        pl.semaphore_signal(barrier, inc=1, device_id=(mod, ahead(step)), device_id_type=MESH)
    pl.semaphore_signal(barrier, inc=1, device_id=(1 - mod, me), device_id_type=MESH)

    sends = [None]
    backs = [None]
    for step in range(1, size):
        sends.append(
            pltpu.make_async_remote_copy(
                src_ref=buf.at[slots_of(step)],
                dst_ref=recv.at[slots_of(step)],
                send_sem=send_sems.at[step],
                recv_sem=recv_sems.at[step],
                device_id=(mod, ahead(step)),
                device_id_type=MESH,
            )
        )
        backs.append(
            pltpu.make_async_remote_copy(
                src_ref=res.at[slots_of(step)],
                dst_ref=back.at[slots_of(step)],
                send_sem=back_send.at[step],
                recv_sem=back_recv.at[step],
                device_id=(mod, behind(step)),
                device_id_type=MESH,
            )
        )

    for copy in small:
        copy.wait()
    experts = expert_ref[...]
    slots = slot_ref[...]
    served = slots < cap
    walk = list(range(near, size)) + list(range(near))
    steps = jnp.zeros_like(experts)
    rank = jnp.zeros_like(experts)
    start = jnp.zeros((1, 1), jnp.int32)
    lost = jnp.zeros((1, 1), jnp.int32)
    lost_rank = jnp.zeros_like(experts)
    for step in walk:
        here = experts == ahead(step)
        steps = jnp.where(here, step, steps)
        rank = jnp.where(here, start + slots, rank)
        lost_rank = jnp.where(here, lost + slots - cap, lost_rank)
        count = jnp.sum(jnp.where(here, 1.0, 0.0), axis=1, keepdims=True).astype(jnp.int32)
        start = start + jnp.minimum(count, cap)
        lost = lost + jnp.maximum(count - cap, 0)
    rank = jnp.where(served, rank, start + lost_rank)
    place_row = jnp.where(served, steps * cap + slots, slot_total)

    lane = lax.broadcasted_iota(jnp.int32, (1, key_count - tokens), 1)
    latent_clip = jnp.where(lane < latents, lane // per_clip, -1)
    token_clip = clip_ref[...] - me * clips
    clip_row = jnp.concatenate([token_clip, latent_clip], axis=1).astype(jnp.float32)

    field = lax.broadcasted_iota(jnp.int32, (16, tokens), 0)
    facts = jnp.where(
        field == 0,
        jnp.where(served, steps, size),
        jnp.where(
            field == 1, jnp.where(served, slots, 0), jnp.where(field == 2, token_clip, 0)
        ),
    ).astype(jnp.float32).astype(jnp.bfloat16)

    gain1 = gain1_ref[...].astype(jnp.float32)
    gain2 = gain2_ref[...].astype(jnp.float32)
    key_clips[...] = to_column(clip_row)
    padding = key_count - row_count
    key_ref[pl.ds(row_count, padding), :] = jnp.zeros((padding, width), jnp.bfloat16)
    rows_ref[pl.ds(tokens, latents), :] = jnp.concatenate(
        [latent_ref[clip].astype(jnp.float32) for clip in range(clips)], axis=0
    ).astype(jnp.bfloat16)
    load_tok.wait()
    load_v.start()
    load_q.start()
    load_proj.start()
    chunk = 48

    def norm1(i, carry):
        here = pl.ds(pl.multiple_of(i * chunk, 16), chunk)
        normed[here, :] = layer_norm(rows_ref[here, :].astype(jnp.float32), gain1).astype(
            jnp.bfloat16
        )
        return carry

    lax.fori_loop(0, row_count // chunk, norm1, 0)

    step_cols = 256

    def project_key(i, carry):
        src = pl.ds(pl.multiple_of(width + i * step_cols, 128), step_cols)
        dst = pl.ds(pl.multiple_of(i * step_cols, 128), step_cols)
        key_ref[pl.ds(0, row_count), dst] = matmul(normed[...], w_qkv[:, src]).astype(jnp.bfloat16)
        return carry

    def project_value(i, carry):
        src = pl.ds(pl.multiple_of(2 * width + i * step_cols, 128), step_cols)
        dst = pl.ds(pl.multiple_of(i * step_cols, 128), step_cols)
        block = matmul(normed[...], w_qkv[:, src]).astype(jnp.bfloat16)
        zeros = jnp.zeros((padding, step_cols), jnp.bfloat16)
        value_t[dst, :] = jnp.transpose(jnp.concatenate([block, zeros], axis=0))
        return carry

    load_k.wait()
    lax.fori_loop(0, width // step_cols, project_key, 0)
    load_v.wait()
    lax.fori_loop(0, width // step_cols, project_value, 0)

    pair = 128 // HEAD

    def attend_few(first):
        here = pl.ds(first, FEW)
        wide = 2 * 128

        def body(i, carry):
            for sub in range(PAIRS):
                at = (i * PAIRS + sub) * wide
                cols = pl.ds(pl.multiple_of(at, 128), wide)
                block = queries[here, cols]
                head_of = lax.broadcasted_iota(jnp.int32, block.shape, 1) // HEAD
                stacked = jnp.concatenate(
                    [
                        jnp.where(head_of == head, block, jnp.zeros_like(block))
                        for head in range(wide // HEAD)
                    ],
                    axis=0,
                )
                scores = lax.dot_general(
                    key_ref[:, cols],
                    stacked,
                    (((1,), (1,)), ((), ())),
                    preferred_element_type=jnp.float32,
                )
                scores = scores + jnp.concatenate([bias[...]] * 2, axis=1)
                weights = jnp.exp(scores - jnp.max(scores, axis=0, keepdims=True))
                norm = jnp.sum(weights, axis=0, keepdims=True)
                summed = matmul(value_t[cols, :], weights.astype(jnp.bfloat16))
                lane_of = lax.broadcasted_iota(jnp.int32, (FEW, 128), 1)
                for j in range(2):
                    part = slice(j * 128, (j + 1) * 128)
                    turned = jnp.transpose(summed[part, part] / norm[:, part])
                    both = jnp.where(lane_of < HEAD, turned[:FEW], turned[FEW:])
                    dst = pl.ds(pl.multiple_of(at + j * 128, 128), 128)
                    attended[here, dst] = both.astype(jnp.bfloat16)
            return carry

        lax.fori_loop(0, width // wide // PAIRS, body, 0)

    def attend(first):
        here = pl.ds(first, EARLY)

        def body(i, carry):
            for sub in range(PAIRS):
                cols = pl.ds(pl.multiple_of((i * PAIRS + sub) * 128, 128), 128)
                block = queries[here, cols]
                head_of = lax.broadcasted_iota(jnp.int32, block.shape, 1) // HEAD
                stacked = jnp.concatenate(
                    [jnp.where(head_of == head, block, jnp.zeros_like(block)) for head in range(pair)],
                    axis=0,
                )
                scores = lax.dot_general(
                    key_ref[:, cols],
                    stacked,
                    (((1,), (1,)), ((), ())),
                    preferred_element_type=jnp.float32,
                )
                scores = scores + jnp.concatenate([bias[...]] * pair, axis=1)
                weights = jnp.exp(scores - jnp.max(scores, axis=0, keepdims=True))
                norm = jnp.sum(weights, axis=0, keepdims=True)
                summed = matmul(value_t[cols, :], weights.astype(jnp.bfloat16))
                heads = [
                    summed[head * HEAD : (head + 1) * HEAD, head * EARLY : (head + 1) * EARLY]
                    / norm[:, head * EARLY : (head + 1) * EARLY]
                    for head in range(pair)
                ]
                attended[here, cols] = jnp.transpose(jnp.concatenate(heads, axis=0)).astype(
                    jnp.bfloat16
                )
            return carry

        lax.fori_loop(0, width // 128 // PAIRS, body, 0)

    inverse_root = jnp.bfloat16(1.0 / math.sqrt(HEAD))

    def project_q(first, rows):
        here = pl.ds(first, rows)

        def body(i, carry):
            cols = pl.ds(pl.multiple_of(i * step_cols, 128), step_cols)
            queries[here, cols] = (
                matmul(attended[here, :], w_qkv[:, cols]).astype(jnp.bfloat16) * inverse_root
            )
            return carry

        lax.fori_loop(0, width // step_cols, body, 0)

    row_in = lax.broadcasted_iota(jnp.int32, (EARLY, 1), 0)

    def gather(first, rows):
        here = pl.ds(first, rows)
        chosen = (first + row_in[:rows]) == rank
        pick = one_hot(chosen)
        moved = lax.dot_general(
            facts, pick, (((1,), (1,)), ((), ())), preferred_element_type=jnp.float32
        )
        row_clips[:, here] = moved[2:3, :]
        moved = moved.astype(jnp.int32)
        at = moved[0:1, :] * cap + moved[1:2, :]
        sorted_place[:, here] = at
        attended[here, :] = matmul(pick, normed[pl.ds(0, tokens), :]).astype(jnp.bfloat16)
        sums[here, :] = matmul(pick, rows_ref[pl.ds(0, tokens), :])

    slot_row = lax.broadcasted_iota(jnp.int32, (128, 1), 0)

    def mask(clips_across):
        bias[...] = jnp.where(key_clips[...] == clips_across, 0.0, -jnp.inf)

    def finish(first, rows):
        here = pl.ds(first, rows)
        if rows == FEW:
            mask(jnp.concatenate([row_clips[:, here]] * 2, axis=1))
            attend_few(first)
        else:
            mask(row_clips[:, here])
            attend(first)
        if first == 0:
            load_proj.wait()

        def project_out(i, carry):
            cols = pl.ds(pl.multiple_of(i * step_cols, 128), step_cols)
            sums[here, cols] += matmul(attended[here, :], w_proj[:, cols])
            return carry

        lax.fori_loop(0, width // step_cols, project_out, 0)
        half = rows // 2
        for part in range(2):
            some = pl.ds(first + part * half, half)
            expert_in[some, :] = layer_norm(sums[some, :], gain2).astype(jnp.bfloat16)

    def dispatch(base, count, known):
        pick = one_hot((base + slot_row[:count]) == sorted_place[:, pl.ds(0, known)])
        buf[pl.ds(base, count), :] = matmul(pick, expert_in[pl.ds(0, known), :]).astype(
            jnp.bfloat16
        )
        for step in range(base // cap, (base + count) // cap):
            if step:
                sends[step].start()
            else:
                recv[slots_of(0), :] = buf[slots_of(0), :]

    pieces = tokens // EARLY
    parts = [(0, FEW), (FEW, FEW)] + [(piece * EARLY, EARLY) for piece in range(1, pieces)]
    load_q.wait()
    gather(0, FEW)
    project_q(0, FEW)
    finish(0, FEW)
    pl.semaphore_wait(barrier, size)
    base = near * cap
    dispatch(base, FEW, FEW)
    load_in.start()
    load_out.start()
    gather(FEW, FEW)
    project_q(FEW, FEW)
    finish(FEW, FEW)
    dispatch(base + FEW, FEW, 2 * FEW)
    gather(EARLY, EARLY)
    project_q(EARLY, EARLY)
    finish(EARLY, EARLY)
    dispatch(base + EARLY, EARLY, 2 * EARLY)
    for first, rows in parts[3:]:
        gather(first, rows)
    attended[pl.ds(tokens, latents), :] = normed[pl.ds(tokens, latents), :]
    attended[pl.ds(row_count, padding), :] = jnp.zeros((padding, width), jnp.bfloat16)
    project_q(2 * EARLY, key_count - 2 * EARLY)
    for first, rows in parts[3:-1]:
        finish(first, rows)
        dispatch(base + first, rows, first + rows)
    finish(*parts[-1])
    base += parts[-1][0]
    for base in list(range(base, slot_total, 128)) + list(range(0, near * cap, 128)):
        count = min(128, slot_total - base, near * cap - base if base < near * cap else 128)
        dispatch(base, count, tokens)

    groups = 4 if size % 4 == 0 else 1
    steps_per = size // groups
    group_rows = steps_per * cap
    tiles = w_in.shape[1] // tile
    for turn, g in enumerate([1, 0, 2, 3] if groups == 4 else [0]):
        for step in range(g * steps_per, (g + 1) * steps_per):
            if step:
                sends[step].wait_recv()
        if turn == 0:
            load_in.wait()
            load_out.wait()
        here = pl.ds(g * group_rows, group_rows)

        def hidden(t):
            cols = pl.ds(pl.multiple_of(t * tile, tile), tile)
            return gelu(matmul(recv[here, :], w_in[:, cols])).astype(jnp.bfloat16)

        def project(t, slot):
            cols = pl.ds(pl.multiple_of(t * tile, tile), tile)
            return matmul(act[slot], w_out[cols, :])

        act[0] = hidden(0)
        acc[...] = jnp.zeros_like(acc)

        def body(t, carry):
            acc[...] += project(t - 1, (t + 1) % 2)
            act[t % 2] = hidden(t)
            return carry

        lax.fori_loop(1, tiles, body, 0)
        res[here, :] = (acc[...] + project(tiles - 1, (tiles - 1) % 2)).astype(jnp.bfloat16)
        for step in range(g * steps_per, (g + 1) * steps_per):
            if step:
                backs[step].start()
            else:
                back[slots_of(0), :] = res[slots_of(0), :]

    tail = pl.ds(tokens, latents)
    mask(latent_clip.astype(jnp.float32))
    attend(tokens)
    my_latent[...] = rows_ref[tail, :].astype(jnp.float32) + matmul(attended[tail, :], w_proj[...])
    latent_copy = pltpu.make_async_remote_copy(
        src_ref=my_latent,
        dst_ref=peer_latent,
        send_sem=lat_sems.at[0],
        recv_sem=lat_sems.at[1],
        device_id=(1 - mod, me),
        device_id_type=MESH,
    )
    latent_copy.start()

    logits = lax.dot_general(
        expert_in[...],
        router_ref[...],
        (((1,), (1,)), ((), ())),
        preferred_element_type=jnp.float32,
    )
    rank_col = to_column(rank.astype(jnp.float32)).astype(jnp.int32)
    places[...] = to_column(place_row.astype(jnp.float32)).astype(jnp.int32)
    expert_col = to_column(experts.astype(jnp.float32)).astype(jnp.int32)
    column = lax.broadcasted_iota(jnp.int32, (EARLY, size), 1)
    sorted_row = lax.broadcasted_iota(jnp.int32, (1, tokens), 1)

    def split(value):
        top = value.astype(jnp.bfloat16)
        return top, value - top.astype(jnp.float32)

    high_logits, rest = split(logits)
    middle_logits, rest = split(rest)
    low_logits, _ = split(rest)
    for piece in range(pieces):
        here = pl.ds(piece * EARLY, EARLY)
        pick = one_hot(rank_col[piece * EARLY : (piece + 1) * EARLY, 0:1] == sorted_row)
        own = (matmul(pick, high_logits) + matmul(pick, middle_logits)) + matmul(pick, low_logits)
        mine = column == expert_col[piece * EARLY : (piece + 1) * EARLY, 0:1]
        picked = jnp.sum(jnp.where(mine, own, 0.0), axis=1, keepdims=True)
        gates[here, :] = jnp.broadcast_to(jax.nn.sigmoid(picked), (EARLY, 128))

        def restore(i, carry):
            cols = pl.ds(pl.multiple_of(i * step_cols, 128), step_cols)
            first, rest = split(sums[:, cols])
            second, rest = split(rest)
            third, _ = split(rest)
            mid[here, cols] = (matmul(pick, first) + matmul(pick, second)) + matmul(pick, third)
            return carry

        lax.fori_loop(0, width // step_cols, restore, 0)

    latent_copy.wait()
    mean = (my_latent[...] + peer_latent[...]) * 0.5
    for clip in range(clips):
        mean_ref[clip] = mean[clip * per_clip : (clip + 1) * per_clip, :].astype(jnp.bfloat16)

    cuts = [0, size // 2, size - size // 4, size] if size % 4 == 0 else [0, size]
    for first, last in zip(cuts[:-1], cuts[1:]):
        for step in range(first, last):
            if step:
                backs[step].wait_recv()
        some = pl.ds(first * cap, (last - first) * cap)

        def combine(i, carry):
            here = pl.ds(pl.multiple_of(i * 128, 128), 128)
            slot = lax.broadcasted_iota(jnp.int32, (1, (last - first) * cap), 1) + first * cap
            pick = one_hot(places[here, 0:1] == slot)
            mixed = mid[here, :] + gates[here, 0:1] * matmul(pick, back[some, :])
            if last == size:
                out_ref[here, :] = mixed.astype(jnp.bfloat16)
            else:
                mid[here, :] = mixed
            return carry

        lax.fori_loop(0, tokens // 128, combine, 0)
    for step in range(1, size):
        sends[step].wait_send()
        backs[step].wait_send()


def layer(
    tokens, bottleneck, clip, expert, slot, gain1, gain2, router, w_qkv, w_proj, w_in, w_out, size
):
    count, width = tokens.shape
    latents = bottleneck.shape[0] * bottleneck.shape[1]
    hidden_width = w_in.shape[1]
    rows = count + latents
    keys = count + 128
    cap = CAP_FACTOR * count // size
    slots = size * cap
    groups = 4 if size % 4 == 0 else 1
    tile = 1024
    vmem = pl.BlockSpec(memory_space=pltpu.VMEM)
    hbm = pl.BlockSpec(memory_space=pl.ANY)
    bf16, f32 = jnp.bfloat16, jnp.float32
    dma = pltpu.SemaphoreType.DMA
    return pl.pallas_call(
        functools.partial(layer_kernel, size, cap, tile),
        out_shape=(
            pltpu.VMEM((count, width), bf16),
            pltpu.VMEM(bottleneck.shape, bf16),
        ),
        in_specs=[hbm] * 12,
        out_specs=(vmem, vmem),
        scratch_shapes=[
            pltpu.VMEM(bottleneck.shape, bf16),
            pltpu.VMEM(clip.shape, jnp.int32),
            pltpu.VMEM(expert.shape, jnp.int32),
            pltpu.VMEM(slot.shape, jnp.int32),
            pltpu.VMEM(gain1.shape, bf16),
            pltpu.VMEM(gain2.shape, bf16),
            pltpu.VMEM(router.shape, bf16),
            pltpu.VMEM((rows, width), bf16),
            pltpu.VMEM((rows, width), bf16),
            pltpu.VMEM((width, 3 * width), bf16),
            pltpu.VMEM((width, width), bf16),
            pltpu.VMEM((width, hidden_width), bf16),
            pltpu.VMEM((hidden_width, width), bf16),
            pltpu.VMEM((keys, width), bf16),
            pltpu.VMEM((width, keys), bf16),
            pltpu.VMEM((keys, 128), f32),
            pltpu.VMEM((keys, width), bf16),
            pltpu.VMEM((keys, width), bf16),
            pltpu.VMEM((keys, EARLY), f32),
            pltpu.VMEM((count, width), f32),
            pltpu.VMEM((count, width), bf16),
            pltpu.VMEM((count, 128), f32),
            pltpu.VMEM((count, 128), jnp.int32),
            pltpu.VMEM((1, count), jnp.int32),
            pltpu.VMEM((1, count), f32),
            pltpu.VMEM((slots, width), bf16),
            pltpu.VMEM((slots, width), bf16),
            pltpu.VMEM((slots, width), bf16),
            pltpu.VMEM((slots, width), bf16),
            pltpu.VMEM((slots // groups, width), f32),
            pltpu.VMEM((2, slots // groups, tile), bf16),
            pltpu.VMEM((count, width), f32),
            pltpu.VMEM((latents, width), f32),
            pltpu.VMEM((latents, width), f32),
            dma(()),
            dma((7,)),
            dma((3,)),
            dma((3,)),
            dma((2,)),
            dma((size,)),
            dma((size,)),
            dma((size,)),
            dma((size,)),
        ],
        compiler_params=pltpu.CompilerParams(
            collective_id=0, has_side_effects=True, vmem_limit_bytes=56 * 1024 * 1024
        ),
    )(tokens, bottleneck, clip, expert, slot, gain1, gain2, router, w_qkv, w_proj, w_in, w_out)


def on_device(
    size,
    tokens,
    bottleneck,
    clip_ids,
    expert_ids,
    slots,
    norm1_gain,
    attn_qkv,
    attn_out,
    norm2_gain,
    router,
    fc_in,
    fc_out,
):
    mixed, latent = layer(
        tokens[0],
        bottleneck,
        clip_ids,
        expert_ids,
        slots,
        norm1_gain,
        norm2_gain,
        router.T,
        attn_qkv[0],
        attn_out[0],
        fc_in[0],
        fc_out[0],
        size,
    )
    return (mixed[None], latent)


def solution(mesh):
    in_specs = (
        P("mod", "exp", None),
        P("exp", None, None),
        P("mod", "exp"),
        P("mod", "exp"),
        P("mod", "exp"),
        P("mod", None),
        P("mod", None, None),
        P("mod", None, None),
        P("mod", None),
        P(),
        P("exp", None, None),
        P("exp", None, None),
    )
    out_specs = (P("mod", "exp", None), P("exp", None, None))
    return jax.shard_map(
        functools.partial(on_device, mesh.shape["exp"]),
        mesh=mesh,
        in_specs=in_specs,
        out_specs=out_specs,
        check_vma=False,
    )
```
